32 devices in a mesh: expert: 8 (over y, x, core), dp: 4 (over z).
Axes of the slice: x: 2, y: 2, z: 4, core: 2. Of those that a mesh axis runs over, the one named last changes fastest.
Arguments:
- gradient: bfloat16 [4, 1, 14336, 2048], P('dp', None, None, 'expert'), may hold values from -6 to 6
- momentum: float32 [4, 1, 14336, 2048], P('dp', None, 'expert'), may hold values from -6 to 6
- group_index: int32 [224, 32, 4, 32], P('expert'), may hold values from 0 to 4095, all different within a row
Outputs:
- momentum_next: float32 [4, 1, 14336, 2048], P('dp', None, 'expert')
- update: float32 [1, 14336, 2048], P(None, None, 'expert')
The draws below stay inside these ranges and needn't reach their ends.
Inputs may be any that keep to these rules, and one draw needn't show every extreme that they name: `group_index`: an entry names the coefficient at row frequency (entry // 64) and column frequency (entry % 64) of its block; the 32 entries of one block and replica differ.
All inputs are finite; a program needn't handle non-finite values.
Results may differ from the reference program's by a relative error of at most 0.0003.
Values may be sent and summed in bfloat16 or wider, within the bound.
No kernel may reach another device: no remote copies, remote signals or barrier semaphores. Data moves between devices by JAX's collectives and lax.ppermute only.
A program may use at most 192 MiB of HBM per device.

```python
import math
import jax
import jax.numpy as jnp
from jax import lax

D = 2048
FF = 14336
EXP = 1
SPAN = 64
TOPK = 32
REPL = 4
NCR = 224
NCC = 32
N_DP = 4


def block_scale(key, extent, split, low, largest):
    def one(dim, shards_of):
        heights = jax.random.uniform(jax.random.fold_in(jax.random.fold_in(key, 6), dim), (shards_of,), jnp.float32, low / len(split), largest / len(split))
        return jnp.repeat(jnp.exp(heights), extent[dim] // shards_of).reshape((-1,) + (1,) * (len(extent) - dim - 1))

    level = one(*split[0])
    for cut in split[1:]:
        level = level * one(*cut)
    return level


def choose_distinct(key, rows, number_of, top, lift):
    order = jax.random.permutation(jax.random.fold_in(key, 1), number_of)
    boost = order
    for power in range(3):
        boost = boost * boost // number_of
    boost = boost * lift // number_of
    chance = jax.random.randint(jax.random.fold_in(key, 2), (rows, number_of), 0, 4096) + boost
    fixed_rows = jax.random.permutation(jax.random.fold_in(key, 3), rows)[jnp.arange(number_of) % rows]
    chance = jnp.where(jnp.arange(rows)[:, None] == fixed_rows[None, :], 1 << 14, chance)
    merit = chance * number_of + jnp.arange(number_of)
    return lax.top_k(merit.astype(jnp.int32), top)[1].astype(jnp.int32)


def bell_draw(rng, dims, width, bound, cuts=(), kind=jnp.bfloat16):
    entries = jax.random.normal(rng, dims, jnp.float32) * width
    if len(cuts) > 0:
        entries = block_scale(rng, dims, cuts, -0.22, 0.18) * entries
    return jnp.clip(entries, min=-bound, max=bound).astype(kind)


def setup_inputs(seed: int = 0) -> dict:
    splits = jax.random.split(jax.random.key(seed), 4)
    return {
        "gradient": bell_draw(splits[0], (REPL, EXP, FF, D), 1.0, 6.0, ((0, 4), (3, 8))),
        "momentum": bell_draw(splits[1], (REPL, EXP, FF, D), 1.0, 6.0, ((0, 4), (2, 8)), jnp.float32),
        "group_index": choose_distinct(splits[2], NCR * NCC * REPL, SPAN * SPAN, TOPK, 0).reshape((NCR, NCC, REPL, TOPK)),
    }


MOMENTUM_DECAY = 0.999
HIGHEST_PRECISION = lax.Precision.HIGHEST

def cosine_table(order_size):
    frequency = jnp.arange(order_size, dtype=jnp.float32)[:, None]
    position = jnp.arange(order_size, dtype=jnp.float32)[None, :]
    weighting = jnp.where(frequency == 0, math.sqrt(1.0 / order_size), math.sqrt(2.0 / order_size))
    return weighting * jnp.cos(math.pi * (2.0 * position + 1.0) * frequency / (2.0 * order_size))

def reference(gradient, momentum, group_index):
    matrix = cosine_table(SPAN)
    block_rows = EXP * FF // SPAN
    block_cols = D // SPAN
    row_ids = jnp.arange(block_rows, dtype=jnp.int32)[:, None, None]
    col_ids = jnp.arange(block_cols, dtype=jnp.int32)[None, :, None]

    def one_replica(running, inputs):
        grad_part, mom_part, replica = inputs
        decayed = MOMENTUM_DECAY * mom_part + grad_part.astype(jnp.float32)
        blocks = decayed.reshape(block_rows, SPAN, block_cols, SPAN)
        coeffs = jnp.einsum('ui,piqj,vj->pquv', matrix, blocks, matrix, precision=HIGHEST_PRECISION)
        chosen = lax.dynamic_index_in_dim(group_index, replica, 2, keepdims=False)
        marked = jnp.zeros((block_rows, block_cols, SPAN * SPAN), jnp.float32).at[row_ids, col_ids, chosen].set(1.0)
        selected = coeffs * marked.reshape(block_rows, block_cols, SPAN, SPAN)
        restored = jnp.einsum('ui,pquv,vj->piqj', matrix, selected, matrix, precision=HIGHEST_PRECISION)
        return (running + restored.reshape(EXP, FF, D), (blocks - restored).reshape(EXP, FF, D))
    initial = jnp.zeros((EXP, FF, D), jnp.float32)
    replicas = jnp.arange(N_DP, dtype=jnp.int32)
    update, momentum_next = lax.scan(one_replica, initial, (gradient, momentum, replicas))
    return (momentum_next, update)
```

```python
import functools
import math

import jax
import jax.numpy as jnp
import numpy as np
from jax import lax
from jax.experimental import pallas as pl
from jax.experimental.pallas import tpu as pltpu
from jax.sharding import PartitionSpec as P

SPAN = 64
MOMENTUM_DECAY = 0.999
CHUNK_WEIGHTS = (1, 1, 1, 1)

F32 = jnp.float32
BF16 = jnp.bfloat16
NT = (((1,), (1,)), ((), ()))


def cosine_table():
    u = np.arange(SPAN, dtype=np.float64)[:, None]
    i = np.arange(SPAN, dtype=np.float64)[None, :]
    scale = np.where(u == 0, math.sqrt(1.0 / SPAN), math.sqrt(2.0 / SPAN))
    return (scale * np.cos(math.pi * (2 * i + 1) * u / (2 * SPAN))).astype(np.float32)


def split_np(x):
    high = x.astype(jnp.bfloat16)
    low = (x - high.astype(np.float32)).astype(jnp.bfloat16)
    return high, low


def split(x):
    high = x.astype(BF16)
    return high, (x - high.astype(F32)).astype(BF16)


def dot(a, b):
    return jnp.dot(a, b, preferred_element_type=F32)


def dot_nt(a, b):
    return lax.dot_general(a, b, NT, preferred_element_type=F32)


def one_hot(rows, target):
    ids = lax.broadcasted_iota(jnp.int32, (rows, target.shape[1]), 0)
    return jnp.where(ids == target, 1.0, 0.0).astype(BF16)


def row_kernel(steps, topk, grad_ref, mom_ref, index_ref, table_ref, *rest):
    next_ref, vals_ref = rest[-2:]
    width = mom_ref.shape[1]
    entries = index_ref.shape[-1]
    lane_block = lax.broadcasted_iota(jnp.int32, (SPAN, entries), 1) // topk
    zero = jnp.zeros((SPAN, entries), F32)
    for step in range(steps):
        rows = pl.ds(step * SPAN, SPAN)
        picked = index_ref[0, step : step + 1, :]
        hot = jnp.concatenate(
            [one_hot(SPAN, picked // SPAN), one_hot(SPAN, picked % SPAN)], axis=1
        )
        gathered = dot(table_ref[...], hot)
        p = gathered[:SPAN, :entries] + gathered[SPAN:, :entries]
        qh = gathered[:SPAN, entries:]
        ql = gathered[SPAN:, entries:]
        spread = jnp.concatenate(
            [
                jnp.concatenate(
                    [
                        jnp.where(lane_block == block, qh, zero).astype(BF16),
                        jnp.where(lane_block == block, ql, zero).astype(BF16),
                    ],
                    axis=1,
                )
                for block in range(width // SPAN)
            ],
            axis=0,
        )
        decayed = MOMENTUM_DECAY * mom_ref[rows, :] + grad_ref[0, rows, :].astype(F32)
        dh, dl = split(decayed)
        half = dot(jnp.concatenate([dh, dl], axis=0), spread)
        half = half[:SPAN] + half[SPAN:]
        half = half[:, :entries] + half[:, entries:]
        value = jnp.sum(half * p, axis=0, keepdims=True)
        vals_ref[0, step : step + 1, :] = value
        vh, vl = split(p * value)
        both = jnp.concatenate(
            [jnp.concatenate([vh, vh], axis=1), jnp.concatenate([vl, vl], axis=1)], axis=0
        )
        restored = dot_nt(both, spread)
        next_ref[rows, :] = decayed - (restored[:SPAN] + restored[SPAN:])


def update_kernel(steps, topk, index_ref, vals_ref, right_ref, left_ref, *rest):
    out_ref, s_ref = rest[-2:]
    replicas = index_ref.shape[0]
    entries = index_ref.shape[-1]
    width = out_ref.shape[1]
    per = min(2, width // SPAN)
    lanes = per * topk
    groups = width // SPAN // per
    total = replicas * lanes
    inner = (lax.broadcasted_iota(jnp.int32, (1, total), 1) // topk) % per
    sub = lax.broadcasted_iota(jnp.int32, (SPAN, total), 0)
    for group in range(groups):
        part = slice(group * lanes, (group + 1) * lanes)
        index = jnp.concatenate([index_ref[r, 0, :, part] for r in range(replicas)], axis=1)
        value = jnp.concatenate([vals_ref[r, 0, :, part] for r in range(replicas)], axis=1)
        for step in range(steps):
            picked = index[step : step + 1, :]
            vals = value[step : step + 1, :]
            at = sub == picked // SPAN
            placed = jnp.where(at, vals, 0.0)
            ph, pl_ = split(placed)
            hot = one_hot(per * SPAN, picked % SPAN + SPAN * inner)
            both = dot_nt(jnp.concatenate([ph, pl_], axis=0), hot)
            s_ref[pl.ds(step * SPAN, SPAN), group * per * SPAN : (group + 1) * per * SPAN] = (
                both[:SPAN] + both[SPAN:]
            )
    sh, sl = split(s_ref[...])
    x = dot(sh, right_ref[0]) + dot(sl, right_ref[0]) + dot(sh, right_ref[1])
    xh, xl = split(x)
    for step in range(steps):
        rows = slice(step * SPAN, (step + 1) * SPAN)
        stacked = jnp.concatenate([xh[rows], xl[rows], xh[rows]], axis=0)
        out_ref[pl.ds(step * SPAN, SPAN), :] = dot(left_ref[...], stacked)


def on_device(gradient, momentum, group_index, *, experts, replicas):
    topk = group_index.shape[3]
    block_rows = group_index.shape[0]
    all_cols = momentum.shape[3]
    all_rows = gradient.shape[1] * gradient.shape[2]
    own_rows = momentum.shape[1] * momentum.shape[2]
    width = gradient.shape[3]
    blocks = width // SPAN
    entries = blocks * topk

    table = cosine_table()
    th, tl = split_np(table)
    gather_table = jnp.asarray(np.concatenate([th.T, tl.T], axis=0))
    eye = np.eye(blocks, dtype=np.float32)
    right_table = jnp.asarray(
        np.stack([np.kron(eye, t.astype(np.float32)).astype(jnp.bfloat16) for t in (th, tl)])
    )
    left_table = jnp.asarray(np.concatenate([th.T, th.T, tl.T], axis=1))

    weights = CHUNK_WEIGHTS if block_rows % sum(CHUNK_WEIGHTS) == 0 else (1, 1)
    unit = block_rows // sum(weights)
    counts = [unit * w for w in weights]
    starts = [sum(counts[:c]) for c in range(len(counts))]

    grad = gradient.reshape(experts, own_rows, width)
    mom = momentum.reshape(own_rows, all_cols)
    replica = lax.axis_index("dp")
    arranged = group_index.reshape(block_rows, experts, blocks, replicas, topk)
    arranged = arranged.transpose(3, 1, 0, 2, 4).reshape(replicas, experts, block_rows, entries)
    own_index = lax.dynamic_index_in_dim(arranged, replica, 0, keepdims=False)
    all_index = lax.all_to_all(arranged, "expert", split_axis=1, concat_axis=1, tiled=True)

    next_buf = None
    update_buf = None
    for count, start in zip(counts, starts):
        rows = count * SPAN
        step_rows = unit * SPAN
        per = count // unit
        first = start // unit
        received = lax.all_to_all(
            lax.slice_in_dim(grad, start * SPAN, start * SPAN + rows, axis=1),
            "expert",
            split_axis=0,
            concat_axis=0,
            tiled=True,
        )
        index_part = own_index.reshape(experts * (block_rows // unit), unit, entries)
        stride = block_rows // unit
        args = [received, mom, index_part, gather_table]
        in_specs = [
            pl.BlockSpec((1, step_rows, width), lambda r, e: (e, r, 0)),
            pl.BlockSpec((step_rows, width), lambda r, e, first=first: (first + r, e)),
            pl.BlockSpec(
                (1, unit, entries),
                lambda r, e, first=first, stride=stride: (e * stride + first + r, 0, 0),
            ),
            pl.BlockSpec((2 * SPAN, SPAN), lambda r, e: (0, 0)),
        ]
        aliases = {}
        if next_buf is not None:
            args.append(next_buf)
            in_specs.append(pl.BlockSpec(memory_space=pl.ANY))
            aliases = {len(args) - 1: 0}
        next_buf, vals = pl.pallas_call(
            functools.partial(row_kernel, unit, topk),
            grid=(per, experts),
            in_specs=in_specs,
            out_specs=[
                pl.BlockSpec((step_rows, width), lambda r, e, first=first: (first + r, e)),
                pl.BlockSpec((1, unit, entries), lambda r, e, per=per: (e * per + r, 0, 0)),
            ],
            out_shape=[
                jax.ShapeDtypeStruct((own_rows, all_cols), F32),
                jax.ShapeDtypeStruct((experts * per, unit, entries), F32),
            ],
            input_output_aliases=aliases,
            cost_estimate=pl.CostEstimate(
                flops=count * experts * 3 * 2 * 128 * 256 * 256,
                bytes_accessed=rows * all_cols * 10,
                transcendentals=0,
            ),
            name="rows_part",
        )(*args)
        sent = jnp.broadcast_to(vals[None], (replicas,) + vals.shape)
        sent = sent.reshape(replicas * experts, per * unit, entries)
        got = lax.all_to_all(sent, ("dp", "expert"), split_axis=0, concat_axis=0, tiled=True)
        got = got.reshape(replicas, experts * per, unit, entries)
        all_part = all_index.reshape(replicas, experts * stride, unit, entries)
        args = [all_part, got, right_table, left_table]
        in_specs = [
            pl.BlockSpec(
                (replicas, 1, unit, entries),
                lambda e, r, first=first, stride=stride: (0, e * stride + first + r, 0, 0),
            ),
            pl.BlockSpec(
                (replicas, 1, unit, entries), lambda e, r, per=per: (0, e * per + r, 0, 0)
            ),
            pl.BlockSpec((2, width, width), lambda e, r: (0, 0, 0)),
            pl.BlockSpec((SPAN, 3 * SPAN), lambda e, r: (0, 0)),
        ]
        aliases = {}
        if update_buf is not None:
            args.append(update_buf)
            in_specs.append(pl.BlockSpec(memory_space=pl.ANY))
            aliases = {len(args) - 1: 0}
        update_buf = pl.pallas_call(
            functools.partial(update_kernel, unit, topk),
            grid=(experts, per),
            in_specs=in_specs,
            out_specs=pl.BlockSpec(
                (step_rows, width),
                lambda e, r, first=first, stride=stride: (e * stride + first + r, 0),
            ),
            out_shape=jax.ShapeDtypeStruct((all_rows, width), F32),
            scratch_shapes=[pltpu.VMEM((step_rows, width), F32)],
            input_output_aliases=aliases,
            cost_estimate=pl.CostEstimate(
                flops=count * experts * 5 * 2 * 128 * 256 * 256,
                bytes_accessed=count * experts * SPAN * width * 4,
                transcendentals=0,
            ),
            name="update_part",
        )(*args)
    return next_buf.reshape(momentum.shape), update_buf[None]


def solution(mesh):
    placed = (
        P("dp", None, None, "expert"),
        P("dp", None, "expert", None),
        P("expert", None, None, None),
    )
    body = functools.partial(
        on_device, experts=mesh.shape["expert"], replicas=mesh.shape["dp"]
    )
    return jax.shard_map(
        body,
        mesh=mesh,
        in_specs=placed,
        out_specs=(P("dp", None, "expert", None), P(None, None, "expert")),
        check_vma=False,
    )
```

```python
import functools
import math

import jax
import jax.numpy as jnp
import numpy as np
from jax import lax
from jax.experimental import pallas as pl
from jax.experimental.pallas import tpu as pltpu
from jax.sharding import PartitionSpec as P

SPAN = 64
LANES = 128
MOMENTUM_DECAY = 0.999
STEP_BLOCKS = 7

F32 = jnp.float32
BF16 = jnp.bfloat16
NT = (((1,), (1,)), ((), ()))


def cosine_table():
    u = np.arange(SPAN, dtype=np.float64)[:, None]
    i = np.arange(SPAN, dtype=np.float64)[None, :]
    scale = np.where(u == 0, math.sqrt(1.0 / SPAN), math.sqrt(2.0 / SPAN))
    return (scale * np.cos(math.pi * (2 * i + 1) * u / (2 * SPAN))).astype(np.float32)


def split_np(x):
    high = x.astype(jnp.bfloat16)
    low = (x - high.astype(np.float32)).astype(jnp.bfloat16)
    return high, low


def split(x):
    high = x.astype(BF16)
    return high, (x - high.astype(F32)).astype(BF16)


def dot(a, b):
    return jnp.dot(a, b, preferred_element_type=F32)


def dot_nt(a, b):
    return lax.dot_general(a, b, NT, preferred_element_type=F32)


def dot_split(high, low, table_ref):
    return dot(high, table_ref[0]) + dot(low, table_ref[0]) + dot(high, table_ref[1])


def lane_gather(table, lanes):
    index = jnp.broadcast_to(lanes, table.shape)
    return jnp.take_along_axis(table, index, axis=1, mode="promise_in_bounds")


def lane_iota(rows):
    return lax.broadcasted_iota(jnp.int32, (rows, LANES), 1)


def row_kernel(
    topk, where_ref, grad_ref, mom_ref, index_ref, lanes_ref, forward_ref, *rest
):
    next_ref, vals_ref, x_ref = rest[-3:]
    steps = vals_ref.shape[1]
    width = mom_ref.shape[1]
    pair = 2 * topk
    decayed = MOMENTUM_DECAY * mom_ref[...] + grad_ref[...].astype(F32)
    next_ref[...] = decayed
    dh, dl = split(decayed)
    x_ref[...] = dot_split(dh, dl, forward_ref)
    row = lane_iota(1)
    second = (row // topk) % 2
    upper = (row // pair) * SPAN
    for part in range(width // LANES):
        index = index_ref[0, 0, :, part * pair : (part + 1) * pair]
        index = jnp.concatenate([index, index], axis=1)
        cols = slice(part * LANES, (part + 1) * LANES)
        for step in range(steps):
            rows = pl.ds(step * SPAN, SPAN)
            picked = index[step : step + 1, :]
            at_row = picked // SPAN
            at_col = picked % SPAN
            p = lane_gather(lanes_ref[0], at_row)
            chosen = lane_gather(x_ref[rows, cols], at_col + second * SPAN)
            value = jnp.sum(chosen * p, axis=0, keepdims=True)
            vals_ref[0, step : step + 1, part * pair : (part + 1) * pair] = value[:, :pair]
            q = lane_gather(lanes_ref[1], at_col + upper)
            spread = jnp.concatenate(
                [jnp.where(second == 0, q, 0.0), jnp.where(second == 1, q, 0.0)], axis=0
            ).astype(BF16)
            vh, vl = split(p * value)
            restored = dot_nt(jnp.concatenate([vh, vl], axis=0), spread)
            next_ref[rows, cols] = next_ref[rows, cols] - (restored[:SPAN] + restored[SPAN:])


def update_kernel(topk, replicas, where_ref, *refs):
    index_refs = refs[:replicas]
    vals_refs = refs[replicas : 2 * replicas]
    lanes_ref, inverse_ref = refs[2 * replicas : 2 * replicas + 2]
    out_ref, zh_ref, zl_ref = refs[-3:]
    steps = vals_refs[0].shape[1]
    width = out_ref.shape[1]
    pair = 2 * topk
    total = replicas * pair
    inner = (lax.broadcasted_iota(jnp.int32, (1, total), 1) // topk) % 2
    sub = lax.broadcasted_iota(jnp.int32, (LANES, total), 0)
    for part in range(width // LANES):
        lanes = slice(part * pair, (part + 1) * pair)
        cols = slice(part * LANES, (part + 1) * LANES)
        index = jnp.concatenate([r[0, 0, 0, :, lanes] for r in index_refs], axis=1)
        value = jnp.concatenate([r[0, :, lanes] for r in vals_refs], axis=1)
        for step in range(steps):
            picked = index[step : step + 1, :]
            vals = value[step : step + 1, :]
            at_row = picked // SPAN
            p = jnp.concatenate(
                [
                    lane_gather(lanes_ref[0], at_row[:, t : t + LANES])
                    for t in range(0, total, LANES)
                ],
                axis=1,
            )
            vh, vl = split(p * vals)
            hot = jnp.where(sub == picked % SPAN + SPAN * inner, 1.0, 0.0).astype(BF16)
            both = dot_nt(jnp.concatenate([vh, vl], axis=0), hot)
            zh, zl = split(both[:SPAN] + both[SPAN:])
            rows = pl.ds(step * SPAN, SPAN)
            zh_ref[rows, cols] = zh
            zl_ref[rows, cols] = zl
    out_ref[...] = dot_split(zh_ref[...], zl_ref[...], inverse_ref)


def on_device(gradient, momentum, group_index, *, experts, replicas):
    topk = group_index.shape[3]
    block_rows = group_index.shape[0]
    all_cols = momentum.shape[3]
    all_rows = gradient.shape[1] * gradient.shape[2]
    own_rows = momentum.shape[1] * momentum.shape[2]
    width = gradient.shape[3]
    blocks = width // SPAN
    entries = blocks * topk
    unit = STEP_BLOCKS
    units = block_rows // unit
    step_rows = unit * SPAN

    table = cosine_table()
    th, tl = split_np(table)
    wide = lambda a, b: np.concatenate([a.astype(np.float32).T, b.astype(np.float32).T], axis=1)
    lane_tables = jnp.asarray(np.stack([wide(table, table), wide(th, tl)]))
    eye = np.eye(blocks, dtype=np.float32)
    kron = lambda t: np.kron(eye, t.astype(np.float32)).astype(jnp.bfloat16)
    forward_tables = jnp.asarray(np.stack([kron(th.T), kron(tl.T)]))
    inverse_tables = jnp.asarray(np.stack([kron(th), kron(tl)]))

    grad = gradient.reshape(experts, own_rows, width)
    mom = momentum.reshape(own_rows, all_cols)
    me = lax.axis_index("expert")
    replica = lax.axis_index("dp")
    order = sorted(range(experts), key=lambda s: (bin(s >> 1).count("1"), s & 1, s))
    arranged = group_index.reshape(block_rows, experts, blocks, replicas, topk)
    arranged = arranged.transpose(3, 1, 0, 2, 4).reshape(replicas, experts, block_rows, entries)
    received = {}
    for s in order:
        part = lax.dynamic_index_in_dim(grad, me ^ s, 0, keepdims=False)
        if s:
            part = lax.ppermute(part, "expert", [(i, i ^ s) for i in range(experts)])
        received[s] = part
    all_index = lax.all_to_all(arranged, "expert", split_axis=1, concat_axis=1, tiled=True)
    own_tiles = arranged.reshape(replicas, experts * units, unit, entries)
    all_tiles = all_index.reshape(replicas, experts * units, unit, entries)

    next_buf = None
    update_buf = None
    half = experts // 2
    groups = (order[:half], order[half:])
    for group in groups:
        kept = {}
        for s in group:
            where = jnp.stack([me ^ s, replica]).astype(jnp.int32)
            args = [where, received[s], mom, own_tiles, lane_tables, forward_tables]
            in_specs = [
                pl.BlockSpec((step_rows, width), lambda i, w: (i, 0)),
                pl.BlockSpec((step_rows, width), lambda i, w: (i, w[0])),
                pl.BlockSpec(
                    (1, 1, unit, entries), lambda i, w: (w[1], w[0] * units + i, 0, 0)
                ),
                pl.BlockSpec((2, SPAN, LANES), lambda i, w: (0, 0, 0)),
                pl.BlockSpec((2, width, width), lambda i, w: (0, 0, 0)),
            ]
            aliases = {}
            if next_buf is not None:
                args.append(next_buf)
                in_specs.append(pl.BlockSpec(memory_space=pl.ANY))
                aliases = {len(args) - 1: 0}
            next_buf, kept[s] = pl.pallas_call(
                functools.partial(row_kernel, topk),
                grid_spec=pltpu.PrefetchScalarGridSpec(
                    num_scalar_prefetch=1,
                    grid=(units,),
                    in_specs=in_specs,
                    out_specs=[
                        pl.BlockSpec((step_rows, width), lambda i, w: (i, w[0])),
                        pl.BlockSpec((1, unit, entries), lambda i, w: (i, 0, 0)),
                    ],
                    scratch_shapes=[pltpu.VMEM((step_rows, width), F32)],
                ),
                out_shape=[
                    jax.ShapeDtypeStruct((own_rows, all_cols), F32),
                    jax.ShapeDtypeStruct((units, unit, entries), F32),
                ],
                input_output_aliases=aliases,
                cost_estimate=pl.CostEstimate(
                    flops=own_rows * width * 2 * 3000,
                    bytes_accessed=own_rows * width * 10,
                    transcendentals=0,
                ),
                name=f"rows_{s}",
            )(*args)
        zero = jnp.zeros((units, unit, entries), F32)
        by_shift = jnp.stack([kept.get(s, zero) for s in range(experts)])
        by_expert = by_shift[me ^ jnp.arange(experts)]
        sent = jnp.broadcast_to(by_expert[:, None], (experts, replicas) + zero.shape)
        sent = sent.reshape((experts * replicas,) + zero.shape)
        got = lax.all_to_all(sent, ("expert", "dp"), split_axis=0, concat_axis=0, tiled=True)
        got = got.reshape(experts * replicas * units, unit, entries)
        group_of = jnp.array(group, jnp.int32) ^ me
        args = [group_of] + [all_tiles] * replicas + [got] * replicas
        args += [lane_tables, inverse_tables]
        in_specs = [
            pl.BlockSpec(
                (1, 1, 1, unit, entries),
                lambda s, i, w, r=r: (0, r, w[s] * units + i, 0, 0),
            )
            for r in range(replicas)
        ]
        in_specs += [
            pl.BlockSpec(
                (1, unit, entries),
                lambda s, i, w, r=r: ((w[s] * replicas + r) * units + i, 0, 0),
            )
            for r in range(replicas)
        ]
        in_specs += [
            pl.BlockSpec((2, SPAN, LANES), lambda s, i, w: (0, 0, 0)),
            pl.BlockSpec((2, width, width), lambda s, i, w: (0, 0, 0)),
        ]
        args[1 : 1 + replicas] = [all_tiles[None]] * replicas
        aliases = {}
        if update_buf is not None:
            args.append(update_buf)
            in_specs.append(pl.BlockSpec(memory_space=pl.ANY))
            aliases = {len(args) - 1: 0}
        update_buf = pl.pallas_call(
            functools.partial(update_kernel, topk, replicas),
            grid_spec=pltpu.PrefetchScalarGridSpec(
                num_scalar_prefetch=1,
                grid=(len(group), units),
                in_specs=in_specs,
                out_specs=pl.BlockSpec((step_rows, width), lambda s, i, w: (w[s] * units + i, 0)),
                scratch_shapes=[
                    pltpu.VMEM((step_rows, width), BF16),
                    pltpu.VMEM((step_rows, width), BF16),
                ],
            ),
            out_shape=jax.ShapeDtypeStruct((all_rows, width), F32),
            input_output_aliases=aliases,
            cost_estimate=pl.CostEstimate(
                flops=len(group) * own_rows * width * 2 * 4000,
                bytes_accessed=len(group) * own_rows * width * 4,
                transcendentals=0,
            ),
            name=f"update_{len(group)}_{group[0]}",
        )(*args)
    return next_buf.reshape(momentum.shape), update_buf[None]


def solution(mesh):
    placed = (
        P("dp", None, None, "expert"),
        P("dp", None, "expert", None),
        P("expert", None, None, None),
    )
    body = functools.partial(
        on_device, experts=mesh.shape["expert"], replicas=mesh.shape["dp"]
    )
    return jax.shard_map(
        body,
        mesh=mesh,
        in_specs=placed,
        out_specs=(P("dp", None, "expert", None), P(None, None, "expert")),
        check_vma=False,
    )
```
